128 devices in a mesh: dp: 16 (over y, z), tensor: 8 (over x, core).
Axes of the slice: x: 4, y: 4, z: 4, core: 2. Of those that a mesh axis runs over, the one named last changes fastest.
Arguments:
- hidden: bfloat16 [8192, 5120], P('dp'), may hold values from -48 to 48
- head_weight: bfloat16 [5120, 8192], P(None, 'tensor'), may hold values from -0.069877124 to 0.069877124
- token_ids: int32 [8192], P('dp'), may hold values from 0 to 8191
- old_logprob: float32 [8192], P('dp'), may hold values from -12.5 to 0.3
- rewards: int32 [128], P('dp'), may hold values from 0 to 1, as said below
- lengths: int32 [128], P('dp'), may hold values from 1 to 64, as said below
- group_ids: int32 [128], P('dp'), may hold values from 0 to 7, as said below
- loss_scale: float32 [], replicated, may hold values from 8192 to 32768
Outputs:
- loss: float32 [], replicated
- grad_hidden: float32 [8192, 5120], P('dp', 'tensor')
- grad_weight: float32 [5120, 8192], P('dp', 'tensor')
The draws below stay inside these ranges and needn't reach their ends.
Inputs may be any that keep to these rules, and one draw needn't show every extreme that they name: `group_ids`: each group number names exactly 16 rollouts. `rewards`: some group holds both a 0 and a 1. `lengths`: some index of dp holds only rollouts of length 64 whose prompts hold both a 0 and a 1.
All inputs are finite; a program needn't handle non-finite values.
Results may differ from the reference program's by a relative error of at most 0.003.
Values may be sent and summed in bfloat16 or wider, within the bound.
A program may use at most 192 MiB of HBM per device.

```python
import math
import jax
import jax.numpy as jnp
from jax import lax

D = 5120
ROLL_DEV = 8
RESP = 64
GROUP = 16
VOCAB = 8192
ROLLOUTS = 128
GROUPS = 8
TOKENS = 8192


def weight_table(key):
    branch_key = jax.random.fold_in(key, 101)
    weight_grid = jnp.clip(jax.random.normal(branch_key, (D, VOCAB), jnp.float32), -5.0, 5.0)
    return weight_grid * D ** (-0.5)


def token_table(key):
    branch_key = jax.random.fold_in(key, 202)
    first_draw = jax.random.randint(jax.random.fold_in(branch_key, 1), (TOKENS,), 0, VOCAB)
    second_draw = jax.random.randint(jax.random.fold_in(branch_key, 2), (TOKENS,), 1, VOCAB + 1)
    return (first_draw * second_draw // VOCAB).astype(jnp.int32)


def group_table(key):
    branch_key = jax.random.fold_in(key, 505)
    device_count = ROLLOUTS // ROLL_DEV
    forced_device = jax.random.randint(jax.random.fold_in(branch_key, 5), (), 0, device_count)
    roll_index = jnp.arange(ROLLOUTS, dtype=jnp.int32)
    in_forced = roll_index // ROLL_DEV == forced_device
    order_key = jax.random.permutation(jax.random.fold_in(branch_key, 1), ROLLOUTS).astype(jnp.int32)
    order_key = order_key + jnp.where(in_forced, 0, ROLLOUTS).astype(jnp.int32)
    ordering = jnp.argsort(order_key, stable=True).astype(jnp.int32)
    rank = jnp.argsort(ordering, stable=True).astype(jnp.int32)
    rank_group = (rank // GROUP).astype(jnp.int32)
    group_of = rank_group
    group_kind = jax.random.randint(jax.random.fold_in(branch_key, 2), (GROUPS,), 0, 4)
    dead_kind = jax.random.randint(jax.random.fold_in(branch_key, 3), (), 0, 2)
    group_index = jnp.arange(GROUPS, dtype=jnp.int32)
    group_kind = jnp.where(group_index == 0, 2, jnp.where(group_index == 1, dead_kind, group_kind))
    group_kind = jnp.where(group_index == GROUPS - 1, 3, group_kind)
    coin_flip = jax.random.randint(jax.random.fold_in(branch_key, 4), (ROLLOUTS,), 0, 2)
    slot_in_group = rank % GROUP
    roll_kind = group_kind[rank_group]
    mixed = jnp.where(slot_in_group == 0, 1, jnp.where(slot_in_group == 1, 0, coin_flip))
    reward_values = jnp.where(roll_kind == 0, 0, jnp.where(roll_kind == 1, 1, mixed))
    return (group_of, reward_values.astype(jnp.int32), in_forced)


def draw_head_weight(key, part):
    return weight_table(key).astype(jnp.bfloat16)


def draw_token_ids(key, part):
    return token_table(key)


def draw_group_ids(key, part):
    return group_table(key)[0]


def draw_rewards(key, part):
    return group_table(key)[1]


def draw_lengths(key, part):
    in_forced = group_table(key)[2]
    random_lengths = jax.random.randint(jax.random.fold_in(key, 707), (ROLLOUTS,), 1, RESP + 1)
    return jnp.where(in_forced, RESP, random_lengths).astype(jnp.int32)


def draw_hidden(key, part):
    branch_key = jax.random.fold_in(key, 303)
    values_out = jnp.clip(jax.random.normal(branch_key, (TOKENS, D), jnp.float32), -5.0, 5.0)
    return values_out.astype(jnp.bfloat16)


def draw_old_logprob(key, part):
    branch_key = jax.random.fold_in(key, 404)
    values_out = -9.5 + jnp.clip(jax.random.normal(branch_key, (TOKENS,), jnp.float32), -2.5, 2.5)
    return values_out


def setup_inputs(seed: int = 0) -> dict:
    arg_keys = jax.random.split(jax.random.key(seed), 9)
    hidden = draw_hidden(jax.random.fold_in(arg_keys[8], 71), 0)
    head_weight = draw_head_weight(jax.random.fold_in(arg_keys[8], 71), 0)
    token_ids = draw_token_ids(jax.random.fold_in(arg_keys[8], 71), 0)
    old_logprob = draw_old_logprob(jax.random.fold_in(arg_keys[8], 71), 0)
    rewards = draw_rewards(jax.random.fold_in(arg_keys[8], 71), 0)
    lengths = draw_lengths(jax.random.fold_in(arg_keys[8], 71), 0)
    group_ids = draw_group_ids(jax.random.fold_in(arg_keys[8], 71), 0)
    loss_scale = jnp.clip(jnp.exp(jax.random.uniform(arg_keys[7], (), jnp.float32, math.log(8192.0), math.log(32768.0))), 8192.0, 32768.0)
    return {"hidden": hidden, "head_weight": head_weight, "token_ids": token_ids, "old_logprob": old_logprob, "rewards": rewards, "lengths": lengths, "group_ids": group_ids, "loss_scale": loss_scale}


clip_low = 0.2
clip_high = 0.28

def group_terms(member, group_wins, reward_float):
    group_alive = jnp.logical_and(group_wins > 0.5, group_wins < GROUP - 0.5).astype(jnp.float32)
    center = group_wins / GROUP
    spread = jnp.where(group_alive > 0.5, jnp.sqrt(group_wins * (GROUP - group_wins)) / GROUP, 1.0)
    roll_alive = lax.optimization_barrier(jnp.sum(member * group_alive[None, :], axis=1))
    roll_center = lax.optimization_barrier(jnp.sum(member * center[None, :], axis=1))
    roll_spread = lax.optimization_barrier(jnp.sum(member * spread[None, :], axis=1))
    advantage = roll_alive * (reward_float - roll_center) / roll_spread
    return (group_alive, roll_alive, advantage)

def policy_terms(log_prob, old_rows, adv_rows, weight_rows, factor):
    prob_ratio = jnp.exp(log_prob - old_rows)
    clipped = jnp.clip(prob_ratio, 1.0 - clip_low, 1.0 + clip_high)
    token_loss = -jnp.minimum(prob_ratio * adv_rows, clipped * adv_rows)
    active = prob_ratio * adv_rows <= clipped * adv_rows
    coefficient = jnp.where(active, -adv_rows * prob_ratio, 0.0) * weight_rows * factor
    return (token_loss, coefficient)

def reference(hidden, head_weight, token_ids, old_logprob, rewards, lengths, group_ids, loss_scale):
    member = (group_ids[:, None] == jnp.arange(GROUPS, dtype=jnp.int32)[None, :]).astype(jnp.float32)
    reward_float = rewards.astype(jnp.float32)
    length_float = lengths.astype(jnp.float32)
    group_wins = lax.optimization_barrier(jnp.sum(member * reward_float[:, None], axis=0))
    group_alive, roll_alive, advantage = group_terms(member, group_wins, reward_float)
    token_count = jnp.sum(roll_alive * length_float)
    divisor = jnp.maximum(token_count, 1.0)
    factor = loss_scale / divisor
    position = jnp.arange(RESP, dtype=jnp.int32)
    inside = (position[None, :] < lengths[:, None]).astype(jnp.float32)
    token_weight = (roll_alive[:, None] * inside).reshape(TOKENS)
    token_adv = jnp.broadcast_to(advantage[:, None], (ROLLOUTS, RESP)).reshape(TOKENS)
    block_rows = math.gcd(TOKENS, 1024)
    block_count = TOKENS // block_rows
    column = jnp.arange(VOCAB, dtype=jnp.int32)[None, :]

    def one_block(carried, inputs):
        grad_table, loss_sum = carried
        row_hidden, row_tokens, row_old, row_weight, row_adv = inputs
        logits = jnp.dot(row_hidden, head_weight, preferred_element_type=jnp.float32)
        row_top = lax.optimization_barrier(jnp.max(logits, axis=1))
        shifted = jnp.exp(logits - row_top[:, None])
        row_total = lax.optimization_barrier(jnp.sum(shifted, axis=1))
        is_target = column == row_tokens[:, None]
        target = lax.optimization_barrier(jnp.sum(jnp.where(is_target, logits, 0.0), axis=1))
        softmax_rows = shifted / row_total[:, None]
        log_prob = target - row_top - jnp.log(row_total)
        token_loss, coefficient = policy_terms(log_prob, row_old, row_adv, row_weight, factor)
        logit_grad = (coefficient[:, None] * (is_target.astype(jnp.float32) - softmax_rows)).astype(jnp.bfloat16)
        grad_rows = jnp.dot(logit_grad, head_weight.T, preferred_element_type=jnp.float32)
        grad_table = grad_table + jnp.dot(row_hidden.T, logit_grad, preferred_element_type=jnp.float32)
        return ((grad_table, loss_sum + jnp.sum(row_weight * token_loss)), grad_rows)
    inputs = (hidden.reshape(block_count, block_rows, D), token_ids.reshape(block_count, block_rows), old_logprob.reshape(block_count, block_rows), token_weight.reshape(block_count, block_rows), token_adv.reshape(block_count, block_rows))
    initial = (jnp.zeros((D, VOCAB), jnp.float32), jnp.zeros((), jnp.float32))
    final_state, stacked = lax.scan(one_block, initial, inputs)
    grad_table, loss_sum = final_state
    return (loss_sum / divisor, stacked.reshape(TOKENS, D), grad_table)
```

```python
import functools

import jax
import jax.numpy as jnp
from jax import lax
from jax.experimental import pallas as pl
from jax.experimental.pallas import tpu as pltpu
from jax.sharding import PartitionSpec as P

GROUP = 16
CLIP_LOW = 0.2
CLIP_HIGH = 0.28
RING = 4
CORES = 2
LANES = 128
MESH = pl.DeviceIdType.MESH
F32 = jnp.float32
BF16 = jnp.bfloat16


class Sems:
    sizes = dict(
        group_y=RING,
        group_z=RING,
        loss_y=RING,
        loss_z=RING,
        stats=RING * CORES,
        hid_y=RING,
        hid_x=RING * 2,
        hid_relay=RING,
        hid_core=RING,
        w_core=RING,
        lg_core=RING,
        lg_own=RING * 2,
        lg_relay=RING * 2,
        x_half=2,
        x_side=2,
        z_half=RING * 2,
        z_side=RING * 2,
    )

    def __init__(self, send, recv):
        self.send, self.recv, self.base, at = send, recv, {}, 0
        for name, size in self.sizes.items():
            self.base[name] = at
            at += size

    @classmethod
    def total(cls):
        return sum(cls.sizes.values())

    def of(self, name, index):
        at = self.base[name] + index
        return self.send.at[at], self.recv.at[at]


def contract_last(a, b):
    return lax.dot_general(a, b, (((1,), (1,)), ((), ())), preferred_element_type=F32)


def kernel(
    h_hbm, w_hbm, tok_ref, old_ref, rew_ref, len_ref, gid_ref, scale_ref,
    loss_ref, gh_ref, gw_ref,
    hv, wv, hq, wp, prob, lgg, lgp, ht, asend, tok_col, coef_col, mul_col, stat_col,
    stat_send, stat_recv, group_y, group_z, loss_y, loss_z,
    x_acc, x_opp, x_side, x_half_in, x_side_in,
    z_acc, z_opp, z_side, z_half_in, z_side_in,
    load_sem, send_sem, recv_sem,
):
    tokens, width = hv.shape
    vocab = wv.shape[1]
    chunk = vocab // RING
    half_cols = width // RING // CORES
    z_rows = width // (RING * RING)
    dp, tensor = lax.axis_index("dp"), lax.axis_index("tensor")
    y, z = dp // RING, dp % RING
    x, core = tensor // CORES, tensor % CORES
    sems = Sems(send_sem, recv_sem)
    started = []

    def at_y(k):
        return ((y + k) % RING * RING + z, tensor)

    def at_z(k):
        return (y * RING + (z + k) % RING, tensor)

    def at_x(k):
        return (dp, (x + k) % RING * CORES + core)

    def at_tensor(k):
        return (dp, (tensor + k) % (RING * CORES))

    partner = (dp, x * CORES + 1 - core)

    def remote(src, dst, name, index, device):
        send, recv = sems.of(name, index)
        return pltpu.make_async_remote_copy(
            src_ref=src, dst_ref=dst, send_sem=send, recv_sem=recv, device_id=device, device_id_type=MESH
        )

    def put(src, dst, name, index, device):
        copy = remote(src, dst, name, index, device)
        copy.start()
        started.append(copy)

    def arrived(dst, name, index):
        remote(dst, dst, name, index, partner).wait_recv()

    k_size = 1024
    k_count = width // k_size
    quarter = [
        pltpu.make_async_copy(
            h_hbm.at[
                pl.ds(pl.multiple_of(x * LANES, LANES), LANES),
                pl.ds(pl.multiple_of(q * half_cols * CORES + core * half_cols, LANES), half_cols),
            ],
            hq.at[q],
            load_sem.at[q],
        )
        for q in range(RING)
    ]
    for copy in quarter:
        copy.start()

    def load_pair(k):
        return (
            pltpu.make_async_copy(
                h_hbm.at[:, pl.ds(pl.multiple_of(k * k_size, k_size), k_size)],
                hv.at[:, pl.ds(pl.multiple_of(k * k_size, k_size), k_size)],
                load_sem.at[RING + 2 * k],
            ),
            pltpu.make_async_copy(
                w_hbm.at[pl.ds(pl.multiple_of(k * k_size, k_size), k_size), :],
                wv.at[pl.ds(pl.multiple_of(k * k_size, k_size), k_size), :],
                load_sem.at[RING + 2 * k + 1],
            ),
        )

    for k in range(k_count):
        for copy in load_pair(k):
            copy.start()

    barrier = pltpu.get_barrier_semaphore()
    peers = (
        [at_y(k) for k in range(1, RING)]
        + [at_z(k) for k in range(1, RING)]
        + [at_tensor(k) for k in range(1, RING * CORES)]
    )
    for device in peers:
        pl.semaphore_signal(barrier, inc=1, device_id=device, device_id_type=MESH)
    pl.semaphore_wait(barrier, len(peers))

    rolls = rew_ref.shape[0]
    roll_tokens = tokens // rolls
    lane8 = lax.broadcasted_iota(jnp.int32, (8, LANES), 1)
    row8 = lax.broadcasted_iota(jnp.int32, (8, LANES), 0)
    local = jnp.zeros((8, LANES), F32)
    for i in range(rolls):
        value = jnp.where(row8 == 0, rew_ref[i].astype(F32), len_ref[i].astype(F32))
        local += jnp.where((lane8 == gid_ref[i]) & (row8 < 2), value, 0.0)
    group_y[y] = local

    half = pl.ds(pl.multiple_of(core * half_cols, 16), half_cols)
    for q in range(RING):
        quarter[q].wait()
        for b in range(half_cols // LANES):
            asend[q, b * LANES : (b + 1) * LANES, :] = hq[q, :, b * LANES : (b + 1) * LANES].T
    ht[y, x, half, :] = asend[y]
    for k in range(1, RING):
        put(group_y.at[y], group_y.at[y], "group_y", k, at_y(k))
    for k in (2, 1, 3):
        put(asend.at[(y + k) % RING], ht.at[y, x, half, :], "hid_y", k, at_y(k))

    def share_over_x(j):
        block = ht.at[(y + j) % RING, x, half, :]
        put(block, block, "hid_x", 2 * j, at_x(3))
        put(block, block, "hid_x", 2 * j + 1, at_x(1))

    def relay_over_x(j):
        source = (y + j) % RING
        right_block = ht.at[source, (x + 1) % RING, half, :]
        left_block = ht.at[source, (x + 3) % RING, half, :]
        arrived(right_block, "hid_x", 2 * j)
        arrived(left_block, "hid_x", 2 * j + 1)
        if j < 2:
            put(left_block, left_block, "hid_relay", j, at_x(1))
        else:
            put(right_block, right_block, "hid_relay", j, at_x(3))

    def hand_to_partner(j):
        source = (y + j) % RING
        arrived(ht.at[source, (x + 2) % RING, half, :], "hid_relay", j)
        block = ht.at[source, :, half, :]
        put(block, block, "hid_core", j, partner)

    share_over_x(0)

    tok = tok_ref[...].astype(F32)
    for r in range(tokens // LANES):
        tok_col[r * LANES : (r + 1) * LANES, :] = jnp.broadcast_to(tok[r : r + 1, :], (LANES, LANES)).T

    for k in range(k_count):
        for copy in load_pair(k):
            copy.wait()

        @pl.loop(0, vocab // 256)
        def _(n, k=k):
            cols = pl.ds(pl.multiple_of(n * 256, 256), 256)
            term = jnp.dot(
                hv[:, k * k_size : (k + 1) * k_size],
                wv[k * k_size : (k + 1) * k_size, cols],
                preferred_element_type=F32,
            )
            if k == 0:
                prob[:, cols] = term
            else:
                prob[:, cols] += term

    for q in range(RING):
        rows = pl.ds(pl.multiple_of((q * CORES + 1 - core) * half_cols, 16), half_cols)
        put(wv.at[rows, :], wp.at[q], "w_core", q, partner)

    step = 32
    lane_step = lax.broadcasted_iota(jnp.int32, (step, LANES), 1)
    column = lax.broadcasted_iota(jnp.int32, (step, vocab), 1).astype(F32)
    first_col = (tensor * vocab).astype(F32)

    @pl.loop(0, tokens // step)
    def _(i):
        rows = pl.ds(pl.multiple_of(i * step, step), step)
        block = prob[rows, :]
        top = jnp.max(block, axis=1, keepdims=True)
        shifted = jnp.exp(block - top)
        prob[rows, :] = shifted
        total = jnp.sum(shifted, axis=1, keepdims=True)
        wanted = jnp.tile(tok_col[rows, :], (1, vocab // LANES)) - first_col
        picked = jnp.sum(jnp.where(column == wanted, block, 0.0), axis=1, keepdims=True)
        stat_col[rows, :] = jnp.where(lane_step == 0, top, jnp.where(lane_step == 1, total, picked))

    for r in range(tokens // LANES):
        flipped = stat_col[r * LANES : (r + 1) * LANES, :].T
        for s in range(3):
            stat_send[s * 4 + r : s * 4 + r + 1, :] = flipped[s : s + 1, :]
    stat_send[12:16, :] = jnp.zeros((4, LANES), F32)
    stat_recv[tensor] = stat_send[...]
    for k in range(1, RING * CORES):
        put(stat_send, stat_recv.at[tensor], "stats", k, at_tensor(k))

    for k in range(1, RING):
        arrived(group_y.at[(y + RING - k) % RING], "group_y", k)
    group_z[z] = group_y[0] + group_y[1] + group_y[2] + group_y[3]
    for k in range(1, RING):
        put(group_z.at[z], group_z.at[z], "group_z", k, at_z(k))

    for k in (1, 3, 2):
        arrived(ht.at[(y + RING - k) % RING, x, half, :], "hid_y", k)
        share_over_x(RING - k)

    for k in range(1, RING * CORES):
        arrived(stat_recv.at[(tensor + RING * CORES - k) % (RING * CORES)], "stats", k)
    row_top = stat_recv[0, 0:4, :]
    for q in range(1, RING * CORES):
        row_top = jnp.maximum(row_top, stat_recv[q, 0:4, :])
    row_total = jnp.zeros_like(row_top)
    target = jnp.zeros_like(row_top)
    for q in range(RING * CORES):
        row_total += stat_recv[q, 4:8, :] * jnp.exp(stat_recv[q, 0:4, :] - row_top)
        target += stat_recv[q, 8:12, :]
    own_scale = jnp.exp(stat_send[0:4, :] - row_top)

    for k in range(1, RING):
        arrived(group_z.at[(z + RING - k) % RING], "group_z", k)
    groups = group_z[0] + group_z[1] + group_z[2] + group_z[3]
    group_wins, group_tokens = groups[0:1, :], groups[1:2, :]
    group_alive = ((group_wins > 0.5) & (group_wins < GROUP - 0.5)).astype(F32)
    token_count = jnp.sum(group_alive * group_tokens, axis=1, keepdims=True)
    divisor = jnp.maximum(token_count, 1.0)
    factor = scale_ref[0] / divisor

    lane4 = lax.broadcasted_iota(jnp.int32, (4, LANES), 1)
    row4 = lax.broadcasted_iota(jnp.int32, (4, LANES), 0)
    token_index = row4 * LANES + lane4
    lane1 = lax.broadcasted_iota(jnp.int32, (1, LANES), 1)
    wins = jnp.zeros((4, LANES), F32)
    reward = jnp.zeros((4, LANES), F32)
    length = jnp.zeros((4, LANES), jnp.int32)
    for i in range(rolls):
        mine = (token_index // roll_tokens) == i
        roll_wins = jnp.sum(jnp.where(lane1 == gid_ref[i], group_wins, 0.0), axis=1, keepdims=True)
        wins = jnp.where(mine, roll_wins, wins)
        reward = jnp.where(mine, rew_ref[i].astype(F32), reward)
        length = jnp.where(mine, len_ref[i], length)
    alive = ((wins > 0.5) & (wins < GROUP - 0.5)).astype(F32)
    spread = jnp.where(alive > 0.5, jnp.sqrt(wins * (GROUP - wins)) / GROUP, 1.0)
    token_adv = alive * (reward - wins / GROUP) / spread
    token_weight = jnp.where(token_index % roll_tokens < length, alive, 0.0)

    log_prob = target - row_top - jnp.log(row_total)
    ratio = jnp.exp(log_prob - old_ref[...])
    clipped = jnp.clip(ratio, 1.0 - CLIP_LOW, 1.0 + CLIP_HIGH)
    token_loss = -jnp.minimum(ratio * token_adv, clipped * token_adv)
    active = ratio * token_adv <= clipped * token_adv
    coefficient = jnp.where(active, -token_adv * ratio, 0.0) * token_weight * factor
    multiplier = coefficient * own_scale / row_total
    weighted = jnp.sum(token_weight * token_loss, axis=1, keepdims=True)
    local_loss = weighted[0:1] + weighted[1:2] + weighted[2:3] + weighted[3:4]

    for r in range(tokens // LANES):
        rows = slice(r * LANES, (r + 1) * LANES)
        coef_col[rows, :] = jnp.broadcast_to(coefficient[r : r + 1, :], (LANES, LANES)).T
        mul_col[rows, :] = jnp.broadcast_to(multiplier[r : r + 1, :], (LANES, LANES)).T

    column_chunk = lax.broadcasted_iota(jnp.int32, (64, chunk), 1).astype(F32)

    def send_chunk(n):
        block = lgg.at[y, n]
        put(block, block, "lg_own", 2 * n, at_y(3))
        put(block, block, "lg_own", 2 * n + 1, at_y(1))

    def relay_chunk(n):
        from_right, from_left = lgg.at[(y + 1) % RING, n], lgg.at[(y + 3) % RING, n]
        low, high = pl.ds(0, tokens // 2), pl.ds(tokens // 2, tokens // 2)
        arrived(from_right, "lg_own", 2 * n)
        arrived(from_left, "lg_own", 2 * n + 1)
        put(from_left.at[low], from_left.at[low], "lg_relay", 2 * n, at_y(1))
        put(from_right.at[high], from_right.at[high], "lg_relay", 2 * n + 1, at_y(3))

    for n in range(RING):

        @pl.loop(0, tokens // 64)
        def _(i, n=n):
            rows = pl.ds(pl.multiple_of(i * 64, 64), 64)
            wanted = jnp.tile(tok_col[rows, :], (1, chunk // LANES)) - (first_col + n * chunk)
            coef = jnp.tile(coef_col[rows, :], (1, chunk // LANES))
            mul = jnp.tile(mul_col[rows, :], (1, chunk // LANES))
            grad = jnp.where(column_chunk == wanted, coef, 0.0) - prob[rows, n * chunk : (n + 1) * chunk] * mul
            lgg[y, n, rows, :] = grad.astype(BF16)

        if n < 2:
            send_chunk(n)
        put(lgg.at[y, n], lgp.at[n], "lg_core", n, partner)

    loss_y[y] = jnp.broadcast_to(local_loss, (8, LANES))
    for k in range(1, RING):
        put(loss_y.at[y], loss_y.at[y], "loss_y", k, at_y(k))

    for n in range(RING):
        arrived(lgp.at[n], "lg_core", n)
        arrived(wp.at[n], "w_core", n)

    def hidden_block(offset):
        q = (x + offset) % RING
        rows = pl.ds(pl.multiple_of((q * CORES + core) * half_cols, 16), half_cols)
        result = None
        for n in range(RING):
            cols = slice(n * chunk, (n + 1) * chunk)
            term = contract_last(lgg[y, n], wv[rows, cols]) + contract_last(lgp[n], wp[q, :, cols])
            result = term if result is None else result + term
        return result

    x_opp[...] = hidden_block(2).astype(BF16)
    mid = tokens // 2
    put(x_opp.at[pl.ds(0, mid)], x_half_in.at[0], "x_half", 0, at_x(3))
    put(x_opp.at[pl.ds(mid, mid)], x_half_in.at[1], "x_half", 1, at_x(1))
    for j in (0, 3, 1, 2):
        relay_over_x(j)

    @pl.loop(0, 3)
    def _(j):
        x_acc[j] = hidden_block(j + 3)

    relay_chunk(0)
    send_chunk(2)
    for j in (0, 3, 1, 2):
        hand_to_partner(j)

    arrived(x_half_in.at[0], "x_half", 0)
    x_side[0, 0:mid, :] = (x_acc[0, 0:mid, :] + x_half_in[0].astype(F32)).astype(BF16)
    x_side[0, mid:, :] = x_acc[0, mid:, :].astype(BF16)
    put(x_side.at[0], x_side_in.at[0], "x_side", 0, at_x(3))
    arrived(x_half_in.at[1], "x_half", 1)
    x_side[1, 0:mid, :] = x_acc[2, 0:mid, :].astype(BF16)
    x_side[1, mid:, :] = (x_acc[2, mid:, :] + x_half_in[1].astype(F32)).astype(BF16)
    put(x_side.at[1], x_side_in.at[1], "x_side", 1, at_x(1))

    relay_chunk(1)
    send_chunk(3)
    for j in range(RING):
        other = pl.ds(pl.multiple_of((1 - core) * half_cols, 16), half_cols)
        arrived(ht.at[(y + j) % RING, :, other, :], "hid_core", j)

    low_rows = z_rows // 2

    def weight_block(n, offset):
        rows = pl.ds(pl.multiple_of((z + offset) % RING * z_rows, 16), z_rows)
        result = None
        for s in range(RING):
            for b in range(RING // 2):
                left = jnp.concatenate([ht[s, 2 * b, rows, :], ht[s, 2 * b + 1, rows, :]], axis=1)
                term = jnp.dot(left, lgg[s, n, b * 256 : (b + 1) * 256, :], preferred_element_type=F32)
                result = term if result is None else result + term
        return result

    def weight_chunk(n):
        low, high = pl.ds(0, tokens // 2), pl.ds(tokens // 2, tokens // 2)
        arrived(lgg.at[(y + 2) % RING, n, low], "lg_relay", 2 * n)
        arrived(lgg.at[(y + 2) % RING, n, high], "lg_relay", 2 * n + 1)
        z_opp[n] = weight_block(n, 2).astype(BF16)
        put(z_opp.at[n, pl.ds(0, low_rows)], z_half_in.at[n, 0], "z_half", 2 * n, at_z(3))
        put(z_opp.at[n, pl.ds(low_rows, low_rows)], z_half_in.at[n, 1], "z_half", 2 * n + 1, at_z(1))

        @pl.loop(0, 3)
        def _(j):
            z_acc[n, j] = weight_block(n, j + 3)

    def pass_sides(n):
        arrived(z_half_in.at[n, 0], "z_half", 2 * n)
        z_side[n, 0, 0:low_rows, :] = (z_acc[n, 0, 0:low_rows, :] + z_half_in[n, 0].astype(F32)).astype(BF16)
        z_side[n, 0, low_rows:, :] = z_acc[n, 0, low_rows:, :].astype(BF16)
        put(z_side.at[n, 0], z_side_in.at[n, 0], "z_side", 2 * n, at_z(3))
        arrived(z_half_in.at[n, 1], "z_half", 2 * n + 1)
        z_side[n, 1, 0:low_rows, :] = z_acc[n, 2, 0:low_rows, :].astype(BF16)
        z_side[n, 1, low_rows:, :] = (z_acc[n, 2, low_rows:, :] + z_half_in[n, 1].astype(F32)).astype(BF16)
        put(z_side.at[n, 1], z_side_in.at[n, 1], "z_side", 2 * n + 1, at_z(1))

    def finish_chunk(n):
        arrived(z_side_in.at[n, 0], "z_side", 2 * n)
        arrived(z_side_in.at[n, 1], "z_side", 2 * n + 1)
        gw_ref[:, n * chunk : (n + 1) * chunk] = (
            z_acc[n, 1] + z_side_in[n, 0].astype(F32) + z_side_in[n, 1].astype(F32)
        )

    weight_chunk(0)
    for k in range(1, RING):
        arrived(loss_y.at[(y + RING - k) % RING], "loss_y", k)
    loss_z[z] = loss_y[0] + loss_y[1] + loss_y[2] + loss_y[3]
    for k in range(1, RING):
        put(loss_z.at[z], loss_z.at[z], "loss_z", k, at_z(k))
    relay_chunk(2)
    weight_chunk(1)
    pass_sides(0)
    relay_chunk(3)
    pass_sides(1)

    arrived(x_side_in.at[0], "x_side", 0)
    arrived(x_side_in.at[1], "x_side", 1)
    gh_ref[...] = x_acc[1] + x_side_in[0].astype(F32) + x_side_in[1].astype(F32)

    weight_chunk(2)
    for k in range(1, RING):
        arrived(loss_z.at[(z + RING - k) % RING], "loss_z", k)
    loss_total = loss_z[0] + loss_z[1] + loss_z[2] + loss_z[3]
    loss_ref[...] = loss_total[0:1, 0:1] / divisor
    finish_chunk(0)
    pass_sides(2)
    finish_chunk(1)
    weight_chunk(3)
    finish_chunk(2)
    pass_sides(3)
    finish_chunk(3)
    for copy in started:
        copy.wait_send()


def shards(hidden, head_weight, token_ids, old_logprob, rewards, lengths, group_ids, loss_scale):
    tokens, width = hidden.shape
    vocab = head_weight.shape[1]
    chunk = vocab // RING
    half_cols = width // RING // CORES
    z_rows = width // (RING * RING)
    rows = tokens // LANES
    hbm = pl.BlockSpec(memory_space=pl.ANY)
    vmem = pl.BlockSpec(memory_space=pltpu.VMEM)
    smem = pl.BlockSpec(memory_space=pltpu.SMEM)
    loss, grad_hidden, grad_weight = pl.pallas_call(
        kernel,
        out_shape=(
            jax.ShapeDtypeStruct((1, 1), F32),
            jax.ShapeDtypeStruct((tokens, half_cols), F32),
            jax.ShapeDtypeStruct((z_rows, vocab), F32),
        ),
        in_specs=[hbm, hbm, vmem, vmem, smem, smem, smem, smem],
        out_specs=(vmem, vmem, vmem),
        scratch_shapes=[
            pltpu.VMEM((tokens, width), BF16),
            pltpu.VMEM((width, vocab), BF16),
            pltpu.VMEM((RING, LANES, half_cols), BF16),
            pltpu.VMEM((RING, half_cols, vocab), BF16),
            pltpu.VMEM((tokens, vocab), F32),
            pltpu.VMEM((RING, RING, tokens, chunk), BF16),
            pltpu.VMEM((RING, tokens, chunk), BF16),
            pltpu.VMEM((RING, RING, half_cols * CORES, LANES), BF16),
            pltpu.VMEM((RING, half_cols, LANES), BF16),
            pltpu.VMEM((tokens, LANES), F32),
            pltpu.VMEM((tokens, LANES), F32),
            pltpu.VMEM((tokens, LANES), F32),
            pltpu.VMEM((tokens, LANES), F32),
            pltpu.VMEM((16, LANES), F32),
            pltpu.VMEM((RING * CORES, 16, LANES), F32),
            pltpu.VMEM((RING, 8, LANES), F32),
            pltpu.VMEM((RING, 8, LANES), F32),
            pltpu.VMEM((RING, 8, LANES), F32),
            pltpu.VMEM((RING, 8, LANES), F32),
            pltpu.VMEM((3, tokens, half_cols), F32),
            pltpu.VMEM((tokens, half_cols), BF16),
            pltpu.VMEM((2, tokens, half_cols), BF16),
            pltpu.VMEM((2, tokens // 2, half_cols), BF16),
            pltpu.VMEM((2, tokens, half_cols), BF16),
            pltpu.VMEM((RING, 3, z_rows, chunk), F32),
            pltpu.VMEM((RING, z_rows, chunk), BF16),
            pltpu.VMEM((RING, 2, z_rows, chunk), BF16),
            pltpu.VMEM((RING, 2, z_rows // 2, chunk), BF16),
            pltpu.VMEM((RING, 2, z_rows, chunk), BF16),
            pltpu.SemaphoreType.DMA((RING + 2 * (width // 1024),)),
            pltpu.SemaphoreType.DMA((Sems.total(),)),
            pltpu.SemaphoreType.DMA((Sems.total(),)),
        ],
        compiler_params=pltpu.CompilerParams(
            collective_id=0, has_side_effects=True, vmem_limit_bytes=66_000_000
        ),
        name="policy_step",
    )(
        hidden,
        head_weight,
        token_ids.reshape(rows, LANES),
        old_logprob.reshape(rows, LANES),
        rewards,
        lengths,
        group_ids,
        loss_scale.reshape(1),
    )
    return (loss.reshape(()), grad_hidden, grad_weight)


def solution(mesh):
    return jax.shard_map(
        shards,
        mesh=mesh,
        in_specs=(
            P("dp", None),
            P(None, "tensor"),
            P("dp"),
            P("dp"),
            P("dp"),
            P("dp"),
            P("dp"),
            P(),
        ),
        out_specs=(P(), P("dp", "tensor"), P("dp", "tensor")),
        check_vma=False,
    )
```

```python
import math

import jax
import jax.numpy as jnp
from jax import lax
from jax.experimental import pallas as pl
from jax.experimental.pallas import tpu as pltpu
from jax.sharding import PartitionSpec as P

GROUP = 16
CLIP_LOW = 0.2
CLIP_HIGH = 0.28
RING = 4
CORES = 2
LANES = 128
MESH = pl.DeviceIdType.MESH
PIECES = ((0, 2), (2, 2), (4, 2), (6, 1), (7, 1))
F32 = jnp.float32
BF16 = jnp.bfloat16


class Sems:
    sizes = dict(
        group_y=1,
        group_z=1,
        loss_y=1,
        loss_z=1,
        token_y=1,
        stats=1,
        hid_y=RING,
        hid_x=RING,
        hid_relay=RING,
        hid_core=1,
        w_core=1,
        lg_core=1,
        lg_own=len(PIECES),
        lg_relay=len(PIECES),
        x_half=2,
        x_side=1,
        z_half=len(PIECES) * 2,
        z_side=len(PIECES),
    )
    sends = 6

    def __init__(self, recv):
        self.recv, self.base, at = recv, {}, 0
        for name, size in self.sizes.items():
            self.base[name] = at
            at += size

    @classmethod
    def total(cls):
        return sum(cls.sizes.values())

    def of(self, name, index):
        return self.recv.at[self.base[name] + index]


def contract_last(a, b):
    return lax.dot_general(a, b, (((1,), (1,)), ((), ())), preferred_element_type=F32)


def kernel(
    h_hbm, w_hbm, tok_hbm, old_hbm, rew_ref, len_ref, gid_ref, scale_ref,
    loss_ref, gh_ref, gw_ref,
    tok_ref, old_ref, hv, wv, hq, wp, prob, lgg, lgo, lgx, lgp, ht, asend, tok_col, top_col, coef_col, mul_col, stat_col,
    token_rows, y_cols, stat_send, stat_recv, group_y, group_z, loss_y, loss_z,
    x_acc, x_opp, x_side, x_half_in, x_side_in,
    z_acc, z_opp, z_side, z_half_in, z_side_in, gh_buf, gw_buf,
    load_sem, out_sem, send_sem, recv_sem,
):
    tokens, width = hv.shape
    vocab = wv.shape[1]
    half_cols = width // RING // CORES
    z_rows = width // (RING * RING)
    dp, tensor = lax.axis_index("dp"), lax.axis_index("tensor")
    y, z = dp // RING, dp % RING
    x, core = tensor // CORES, tensor % CORES
    sems = Sems(recv_sem)
    sent = [0] * Sems.sends

    def at_y(k):
        return ((y + k) % RING * RING + z, tensor)

    def at_z(k):
        return (y * RING + (z + k) % RING, tensor)

    def at_x(k):
        return (dp, (x + k) % RING * CORES + core)

    def at_tensor(k):
        return (dp, (tensor + k) % (RING * CORES))

    partner = (dp, x * CORES + 1 - core)

    def size_of(ref):
        return math.prod(ref.shape) * ref.dtype.itemsize

    def wait_for(sem, size):
        ref = tok_col if size <= size_of(tok_col) else wv
        row = size_of(ref) // ref.shape[0]
        assert size % (8 * row) == 0, size
        rows = ref.at[pl.ds(0, size // row)]
        pltpu.make_async_copy(rows, rows, sem).wait()

    def put(src, dst, name, index, device):
        if size_of(src) < 2**14:
            slot = 0
        elif name.startswith("z"):
            slot = 1
        else:
            slot = min(range(2, Sems.sends), key=lambda i: sent[i])
        sent[slot] += size_of(src)
        pltpu.make_async_remote_copy(
            src_ref=src,
            dst_ref=dst,
            send_sem=send_sem.at[slot],
            recv_sem=sems.of(name, index),
            device_id=device,
            device_id_type=MESH,
        ).start()

    def arrived(ref, name, index=0, count=1):
        wait_for(sems.of(name, index), size_of(ref) * count)

    k_size = 1024
    k_count = width // k_size
    quarter = [
        pltpu.make_async_copy(
            h_hbm.at[
                pl.ds(pl.multiple_of(x * LANES, LANES), LANES),
                pl.ds(pl.multiple_of(((y + k) % RING * CORES + core) * half_cols, LANES), half_cols),
            ],
            hq.at[k - 1],
            load_sem.at[0],
        )
        for k in range(1, RING)
    ]
    small = [
        pltpu.make_async_copy(tok_hbm, tok_ref, load_sem.at[1]),
        pltpu.make_async_copy(old_hbm, old_ref, load_sem.at[1]),
    ]
    for copy in small + quarter:
        copy.start()

    def load_pair(k):
        return (
            pltpu.make_async_copy(
                h_hbm.at[:, pl.ds(pl.multiple_of(k * k_size, k_size), k_size)],
                hv.at[:, pl.ds(pl.multiple_of(k * k_size, k_size), k_size)],
                load_sem.at[2 + k],
            ),
            pltpu.make_async_copy(
                w_hbm.at[pl.ds(pl.multiple_of(k * k_size, k_size), k_size), :],
                wv.at[pl.ds(pl.multiple_of(k * k_size, k_size), k_size), :],
                load_sem.at[2 + k],
            ),
        )

    for k in range(k_count):
        for copy in load_pair(k):
            copy.start()

    barrier = pltpu.get_barrier_semaphore()
    peers = (
        [at_y(k) for k in range(1, RING)]
        + [at_z(k) for k in range(1, RING)]
        + [at_tensor(k) for k in range(1, RING * CORES)]
    )
    for device in peers:
        pl.semaphore_signal(barrier, inc=1, device_id=device, device_id_type=MESH)

    rolls = rew_ref.shape[0]
    roll_tokens = tokens // rolls
    lane8 = lax.broadcasted_iota(jnp.int32, (8, LANES), 1)
    row8 = lax.broadcasted_iota(jnp.int32, (8, LANES), 0)
    local = jnp.zeros((8, LANES), F32)
    for i in range(rolls):
        value = jnp.where(row8 == 0, rew_ref[i].astype(F32), len_ref[i].astype(F32))
        local += jnp.where((lane8 == gid_ref[i]) & (row8 < 2), value, 0.0)
    group_y[y] = local

    wait_for(load_sem.at[1], size_of(tok_ref) * 2)
    tok = (tok_ref[...] - tensor * vocab).astype(F32)
    for r in range(tokens // LANES):
        tok_col[r * LANES : (r + 1) * LANES, :] = jnp.broadcast_to(tok[r : r + 1, :], (LANES, LANES)).T

    half = pl.ds(pl.multiple_of(core * half_cols, 16), half_cols)
    wait_for(load_sem.at[0], size_of(hq))
    for k in range(1, RING):
        for b in range(half_cols // LANES):
            asend[k - 1, b * LANES : (b + 1) * LANES, :] = hq[k - 1, :, b * LANES : (b + 1) * LANES].T

    def logits(k):
        wait_for(load_sem.at[2 + k], (tokens + vocab) * k_size * 2)

        @pl.loop(0, vocab // 512)
        def _(n):
            cols = pl.ds(pl.multiple_of(n * 512, 512), 512)
            term = jnp.dot(
                hv[:, k * k_size : (k + 1) * k_size],
                wv[k * k_size : (k + 1) * k_size, cols],
                preferred_element_type=F32,
            )
            if k == 0:
                prob[:, cols] = term
            else:
                prob[:, cols] += term

    def send_weights(q):
        rows = pl.ds(pl.multiple_of((q * CORES + 1 - core) * half_cols, 16), half_cols)
        put(w_hbm.at[rows, :], wp.at[q], "w_core", 0, partner)

    logits(0)
    pl.semaphore_wait(barrier, len(peers))
    for k in range(1, RING):
        put(group_y.at[y], group_y.at[y], "group_y", 0, at_y(k))
    for k in (1, 3, 2):
        put(asend.at[k - 1], ht.at[y, x, half, :], "hid_y", k, at_y(k))
    for q in range(RING):
        send_weights(q)
    for k in range(1, k_count):
        logits(k)
        if k == 3:
            arrived(group_y.at[0], "group_y", count=RING - 1)
            group_z[z] = group_y[0] + group_y[1] + group_y[2] + group_y[3]
            for j in range(1, RING):
                put(group_z.at[z], group_z.at[z], "group_z", 0, at_z(j))

    def share_over_x(j):
        block = ht.at[(y + j) % RING, x, half, :]
        arrived(block, "hid_y", RING - j)
        put(block, block, "hid_x", j, at_x(3))
        put(block, block, "hid_x", j, at_x(1))

    front = pl.ds(pl.multiple_of(core * half_cols, 16), half_cols // 2)
    back = pl.ds(pl.multiple_of(core * half_cols + half_cols // 2, 16), half_cols // 2)

    def relay_over_x(j):
        source = (y + j) % RING
        arrived(ht.at[source, x, half, :], "hid_x", j, 2)
        left_block = ht.at[source, (x + 3) % RING, front, :]
        right_block = ht.at[source, (x + 1) % RING, back, :]
        put(left_block, left_block, "hid_relay", j, at_x(1))
        put(right_block, right_block, "hid_relay", j, at_x(3))

    def hand_to_partner(j):
        source = (y + j) % RING
        if j:
            arrived(ht.at[source, x, half, :], "hid_relay", j)
        block = ht.at[source, :, half, :]
        put(block, block, "hid_core", 0, partner)

    step = 32
    lane_step = lax.broadcasted_iota(jnp.int32, (step, LANES), 1)
    lane_step_f = lane_step.astype(F32)
    pieces = vocab // LANES

    @pl.loop(0, tokens // step, unroll=4)
    def _(i):
        rows = pl.ds(pl.multiple_of(i * step, step), step)
        top = prob[rows, 0:LANES]
        for p in range(1, pieces):
            top = jnp.maximum(top, prob[rows, p * LANES : (p + 1) * LANES])
        top_col[rows, :] = jnp.broadcast_to(jnp.max(top, axis=1, keepdims=True), (step, LANES))

    @pl.loop(0, tokens // step, unroll=4)
    def _(i):
        rows = pl.ds(pl.multiple_of(i * step, step), step)
        top, wanted = top_col[rows, :], tok_col[rows, :]
        total = picked = jnp.zeros((step, LANES), F32)
        for p in range(pieces):
            block = prob[rows, p * LANES : (p + 1) * LANES]
            shifted = jnp.exp(block - top)
            prob[rows, p * LANES : (p + 1) * LANES] = shifted
            lgg[y, p, rows, :] = shifted.astype(BF16)
            total += shifted
            picked += jnp.where(lane_step_f + float(p * LANES) == wanted, block, 0.0)
        total = jnp.sum(total, axis=1, keepdims=True)
        picked = jnp.sum(picked, axis=1, keepdims=True)
        stat_col[rows, :] = jnp.where(lane_step == 0, top, jnp.where(lane_step == 1, total, picked))

    def piece(ref, n):
        first, count = PIECES[n]
        return ref.at[pl.ds(first, count)]

    def send_chunk(n):
        block = piece(lgg.at[y], n)
        put(block, block, "lg_own", n, at_y(3))
        put(block, block, "lg_own", n, at_y(1))

    low, high = pl.ds(0, tokens // 2), pl.ds(tokens // 2, tokens // 2)

    def relay_chunk(n):
        from_right, from_left = piece(lgg.at[(y + 1) % RING], n), piece(lgg.at[(y + 3) % RING], n)
        arrived(from_right, "lg_own", n, 2)
        put(from_left.at[:, low], from_left.at[:, low], "lg_relay", n, at_y(1))
        put(from_right.at[:, high], from_right.at[:, high], "lg_relay", n, at_y(3))

    for n in range(2):
        send_chunk(n)

    for r in range(tokens // LANES):
        flipped = stat_col[r * LANES : (r + 1) * LANES, :].T
        for s in range(3):
            stat_send[s * 4 + r : s * 4 + r + 1, :] = flipped[s : s + 1, :]
    stat_send[12:16, :] = jnp.zeros((4, LANES), F32)
    stat_recv[tensor] = stat_send[...]
    for k in range(1, RING * CORES):
        put(stat_send, stat_recv.at[tensor], "stats", 0, at_tensor(k))

    for j in (1, 3):
        share_over_x(j)

    for b in range(half_cols // LANES):
        cols = pl.ds(pl.multiple_of((y * CORES + core) * half_cols + b * LANES, LANES), LANES)
        rows = pl.ds(pl.multiple_of(core * half_cols + b * LANES, LANES), LANES)
        for q in range(RING):
            ht[y, q, rows, :] = hv[q * LANES : (q + 1) * LANES, cols].T

    arrived(group_z.at[0], "group_z", count=RING - 1)
    groups = group_z[0] + group_z[1] + group_z[2] + group_z[3]
    group_wins, group_tokens = groups[0:1, :], groups[1:2, :]
    group_alive = ((group_wins > 0.5) & (group_wins < GROUP - 0.5)).astype(F32)
    token_count = jnp.sum(group_alive * group_tokens, axis=1, keepdims=True)
    divisor = jnp.maximum(token_count, 1.0)
    factor = scale_ref[0] / divisor

    lane4 = lax.broadcasted_iota(jnp.int32, (4, LANES), 1)
    row4 = lax.broadcasted_iota(jnp.int32, (4, LANES), 0)
    token_index = row4 * LANES + lane4
    lane1 = lax.broadcasted_iota(jnp.int32, (1, LANES), 1)
    wins = jnp.zeros((4, LANES), F32)
    reward = jnp.zeros((4, LANES), F32)
    length = jnp.zeros((4, LANES), jnp.int32)
    for i in range(rolls):
        mine = (token_index // roll_tokens) == i
        roll_wins = jnp.sum(jnp.where(lane1 == gid_ref[i], group_wins, 0.0), axis=1, keepdims=True)
        wins = jnp.where(mine, roll_wins, wins)
        reward = jnp.where(mine, rew_ref[i].astype(F32), reward)
        length = jnp.where(mine, len_ref[i], length)
    alive = ((wins > 0.5) & (wins < GROUP - 0.5)).astype(F32)
    spread = jnp.where(alive > 0.5, jnp.sqrt(wins * (GROUP - wins)) / GROUP, 1.0)
    token_adv = alive * (reward - wins / GROUP) / spread
    token_weight = jnp.where(token_index % roll_tokens < length, alive, 0.0)

    arrived(stat_send, "stats", count=RING * CORES - 1)
    share_over_x(2)
    row_top = stat_recv[0, 0:4, :]
    for q in range(1, RING * CORES):
        row_top = jnp.maximum(row_top, stat_recv[q, 0:4, :])
    row_total = jnp.zeros_like(row_top)
    target = jnp.zeros_like(row_top)
    for q in range(RING * CORES):
        row_total += stat_recv[q, 4:8, :] * jnp.exp(stat_recv[q, 0:4, :] - row_top)
        target += stat_recv[q, 8:12, :]
    own_scale = jnp.exp(stat_send[0:4, :] - row_top)

    log_prob = target - row_top - jnp.log(row_total)
    ratio = jnp.exp(log_prob - old_ref[...])
    clipped = jnp.clip(ratio, 1.0 - CLIP_LOW, 1.0 + CLIP_HIGH)
    token_loss = -jnp.minimum(ratio * token_adv, clipped * token_adv)
    active = ratio * token_adv <= clipped * token_adv
    coefficient = jnp.where(active, -token_adv * ratio, 0.0) * token_weight * factor
    multiplier = coefficient * own_scale / row_total
    weighted = jnp.sum(token_weight * token_loss, axis=1, keepdims=True)
    local_loss = weighted[0:1] + weighted[1:2] + weighted[2:3] + weighted[3:4]

    for r in range(tokens // LANES):
        rows = slice(r * LANES, (r + 1) * LANES)
        coef_col[rows, :] = jnp.broadcast_to(coefficient[r : r + 1, :], (LANES, LANES)).T
        mul_col[rows, :] = jnp.broadcast_to(multiplier[r : r + 1, :], (LANES, LANES)).T

    token_rows[y, 0:4, :] = coefficient
    token_rows[y, 4:8, :] = multiplier
    token_rows[y, 8:12, :] = tok
    token_rows[y, 12:16, :] = jnp.zeros((4, LANES), F32)
    for k in (2, 1, 3):
        put(token_rows.at[y], token_rows.at[y], "token_y", 0, at_y(k))

    lane_lg = lax.broadcasted_iota(jnp.int32, (64, LANES), 1).astype(F32)
    for n, (first, count) in enumerate(PIECES):

        @pl.loop(0, tokens // 64)
        def _(i):
            rows = pl.ds(pl.multiple_of(i * 64, 64), 64)
            wanted, coef, mul = tok_col[rows, :], coef_col[rows, :], mul_col[rows, :]
            for p in range(first, first + count):
                hit = jnp.where(lane_lg + float(p * LANES) == wanted, coef, 0.0)
                lgo[p, rows, :] = (hit - prob[rows, p * LANES : (p + 1) * LANES] * mul).astype(BF16)

        put(piece(lgo, n), piece(lgp, n), "lg_core", 0, partner)

    def token_columns():
        arrived(token_rows.at[0], "token_y", count=RING - 1)
        for k in range(1, RING):
            other = (y + k) % RING
            for r in range(tokens // LANES):
                rows = slice(r * LANES, (r + 1) * LANES)
                for i in range(3):
                    line = token_rows[other, i * 4 + r : i * 4 + r + 1, :]
                    y_cols[k - 1, i, rows, :] = jnp.broadcast_to(line, (LANES, LANES)).T

    def gather_gradients(n):
        first, count = PIECES[n]
        for k in range(1, RING):
            other = (y + k) % RING

            @pl.loop(0, tokens // 64)
            def _(i, k=k, other=other):
                rows = pl.ds(pl.multiple_of(i * 64, 64), 64)
                coef, mul, wanted = y_cols[k - 1, 0, rows, :], y_cols[k - 1, 1, rows, :], y_cols[k - 1, 2, rows, :]
                for p in range(count):
                    hit = jnp.where(lane_lg + float((first + p) * LANES) == wanted, coef, 0.0)
                    lgx[k - 1, p, rows, :] = (hit - lgg[other, first + p, rows, :].astype(F32) * mul).astype(BF16)

    loss_y[y] = jnp.broadcast_to(local_loss, (8, LANES))
    for k in range(1, RING):
        put(loss_y.at[y], loss_y.at[y], "loss_y", 0, at_y(k))

    def weight_rows(offset):
        return pl.ds(pl.multiple_of(((x + offset) % RING * CORES + core) * half_cols, 16), half_cols)

    def pair(ref, p):
        return jnp.concatenate([ref[p], ref[p + 1]], axis=1)

    def hidden_block(offset):
        q, rows = (x + offset) % RING, weight_rows(offset)
        result = None
        for p in range(0, pieces, 2):
            cols = slice(p * LANES, (p + 2) * LANES)
            for term in (contract_last(pair(lgo, p), wv[rows, cols]), contract_last(pair(lgp, p), wp[q, :, cols])):
                result = term if result is None else result + term
        return result

    def hidden_blocks(first, last):
        @pl.loop(first, last)
        def _(j):
            x_acc[j] = hidden_block(j + 2)

    hand_to_partner(0)
    arrived(lgp, "lg_core")
    arrived(wp, "w_core")
    hidden_blocks(0, 2)
    x_opp[...] = x_acc[0].astype(BF16)
    mid = tokens // 2
    relay_over_x(1)
    relay_over_x(3)
    relay_chunk(0)
    send_chunk(2)
    hidden_blocks(2, 4)
    relay_over_x(2)
    put(x_opp.at[pl.ds(0, mid)], x_half_in.at[0], "x_half", 0, at_x(3))
    put(x_opp.at[pl.ds(mid, mid)], x_half_in.at[1], "x_half", 1, at_x(1))
    token_columns()
    relay_chunk(1)
    send_chunk(3)
    for j in (1, 3, 2):
        hand_to_partner(j)
    arrived(ht.at[:, :, half, :], "hid_core")

    low_rows = z_rows // 2

    def weight_block(n, offset):
        first, count = PIECES[n]
        rows = pl.ds(pl.multiple_of((z + offset) % RING * z_rows, 16), z_rows)
        result = None
        for k in range(RING):
            s = (y + k) % RING
            for b in range(RING // 2):
                left = jnp.concatenate([ht[s, 2 * b, rows, :], ht[s, 2 * b + 1, rows, :]], axis=1)
                part = slice(b * 256, (b + 1) * 256)
                right = [lgx[k - 1, p, part, :] if k else lgo[first + p, part, :] for p in range(count)]
                right = right[0] if count == 1 else jnp.concatenate(right, axis=1)
                term = jnp.dot(left, right, preferred_element_type=F32)
                result = term if result is None else result + term
        return result

    def columns(n):
        first, count = PIECES[n]
        return pl.ds(first * LANES, count * LANES)

    def weight_chunk(n):
        from_opposite = piece(lgg.at[(y + 2) % RING], n)
        arrived(from_opposite, "lg_relay", n)
        first, count = PIECES[n]
        gather_gradients(n)
        block = weight_block(n, 2).astype(BF16)
        for p in range(count):
            z_opp[first + p] = block[:, p * LANES : (p + 1) * LANES]
        out = piece(z_opp, n)
        put(out.at[:, pl.ds(0, low_rows)], piece(z_half_in.at[0], n), "z_half", 2 * n, at_z(3))
        put(out.at[:, pl.ds(low_rows, low_rows)], piece(z_half_in.at[1], n), "z_half", 2 * n + 1, at_z(1))

        @pl.loop(0, 3)
        def _(j):
            z_acc[j, :, columns(n)] = weight_block(n, j + 3)

    def pass_sides(n):
        first, count = PIECES[n]
        for side, (j, device) in enumerate(((0, at_z(3)), (2, at_z(1)))):
            arrived(piece(z_half_in.at[side], n), "z_half", 2 * n + side)
            summed = slice(side * low_rows, (side + 1) * low_rows)
            plain = slice((1 - side) * low_rows, (2 - side) * low_rows)
            for p in range(first, first + count):
                cols = slice(p * LANES, (p + 1) * LANES)
                z_side[side, p, summed, :] = (z_acc[j, summed, cols] + z_half_in[side, p].astype(F32)).astype(BF16)
                z_side[side, p, plain, :] = z_acc[j, plain, cols].astype(BF16)
            put(piece(z_side.at[side], n), piece(z_side_in.at[side], n), "z_side", n, device)

    def finish_chunk(n):
        first, count = PIECES[n]
        arrived(piece(z_side_in.at[0], n), "z_side", n, 2)
        for p in range(first, first + count):
            cols = slice(p * LANES, (p + 1) * LANES)
            gw_buf[:, cols] = z_acc[1, :, cols] + z_side_in[0, p].astype(F32) + z_side_in[1, p].astype(F32)
        cols = columns(n)
        copy = pltpu.make_async_copy(gw_buf.at[:, cols], gw_ref.at[:, cols], out_sem.at[0])
        copy.start()

    def pass_x_sides():
        arrived(x_half_in.at[0], "x_half", 0)
        x_side[0, 0:mid, :] = (x_acc[1, 0:mid, :] + x_half_in[0].astype(F32)).astype(BF16)
        x_side[0, mid:, :] = x_acc[1, mid:, :].astype(BF16)
        put(x_side.at[0], x_side_in.at[0], "x_side", 0, at_x(3))
        arrived(x_half_in.at[1], "x_half", 1)
        x_side[1, 0:mid, :] = x_acc[3, 0:mid, :].astype(BF16)
        x_side[1, mid:, :] = (x_acc[3, mid:, :] + x_half_in[1].astype(F32)).astype(BF16)
        put(x_side.at[1], x_side_in.at[1], "x_side", 0, at_x(1))

    def finish_x():
        arrived(x_side_in.at[0], "x_side", 0, 2)
        gh_buf[...] = x_acc[2] + x_side_in[0].astype(F32) + x_side_in[1].astype(F32)
        copy = pltpu.make_async_copy(gh_buf, gh_ref, out_sem.at[0])
        copy.start()

    weight_chunk(0)
    arrived(loss_y.at[0], "loss_y", count=RING - 1)
    loss_z[z] = loss_y[0] + loss_y[1] + loss_y[2] + loss_y[3]
    for k in range(1, RING):
        put(loss_z.at[z], loss_z.at[z], "loss_z", 0, at_z(k))
    relay_chunk(2)
    send_chunk(4)
    weight_chunk(1)
    pass_sides(0)
    pass_x_sides()
    relay_chunk(3)
    weight_chunk(2)
    pass_sides(1)
    relay_chunk(4)
    arrived(loss_z.at[0], "loss_z", count=RING - 1)
    loss_total = loss_z[0] + loss_z[1] + loss_z[2] + loss_z[3]
    weight_chunk(3)
    weight_chunk(4)
    pass_sides(2)
    pass_sides(3)
    pass_sides(4)
    finish_chunk(0)
    finish_chunk(1)
    finish_x()
    finish_chunk(2)
    finish_chunk(3)
    finish_chunk(4)
    loss_ref[...] = loss_total[0:1, 0:1] / divisor
    for slot in range(Sems.sends):
        wait_for(send_sem.at[slot], sent[slot])
    wait_for(out_sem.at[0], size_of(gh_buf) + size_of(gw_buf))


def shards(hidden, head_weight, token_ids, old_logprob, rewards, lengths, group_ids, loss_scale):
    tokens, width = hidden.shape
    vocab = head_weight.shape[1]
    pieces = vocab // LANES
    half_cols = width // RING // CORES
    z_rows = width // (RING * RING)
    rows = tokens // LANES
    hbm = pl.BlockSpec(memory_space=pl.ANY)
    vmem = pl.BlockSpec(memory_space=pltpu.VMEM)
    smem = pl.BlockSpec(memory_space=pltpu.SMEM)
    loss, grad_hidden, grad_weight = pl.pallas_call(
        kernel,
        out_shape=(
            jax.ShapeDtypeStruct((1, 1), F32),
            jax.ShapeDtypeStruct((tokens, half_cols), F32),
            jax.ShapeDtypeStruct((z_rows, vocab), F32),
        ),
        in_specs=[hbm, hbm, hbm, hbm, smem, smem, smem, smem],
        out_specs=(vmem, hbm, hbm),
        scratch_shapes=[
            pltpu.VMEM((rows, LANES), jnp.int32),
            pltpu.VMEM((rows, LANES), F32),
            pltpu.VMEM((tokens, width), BF16),
            pltpu.VMEM((width, vocab), BF16),
            pltpu.VMEM((RING - 1, LANES, half_cols), BF16),
            pltpu.VMEM((RING, half_cols, vocab), BF16),
            pltpu.VMEM((tokens, vocab), F32),
            pltpu.VMEM((RING, pieces, tokens, LANES), BF16),
            pltpu.VMEM((pieces, tokens, LANES), BF16),
            pltpu.VMEM((RING - 1, 2, tokens, LANES), BF16),
            pltpu.VMEM((pieces, tokens, LANES), BF16),
            pltpu.VMEM((RING, RING, half_cols * CORES, LANES), BF16),
            pltpu.VMEM((RING - 1, half_cols, LANES), BF16),
            pltpu.VMEM((tokens, LANES), F32),
            pltpu.VMEM((tokens, LANES), F32),
            pltpu.VMEM((tokens, LANES), F32),
            pltpu.VMEM((tokens, LANES), F32),
            pltpu.VMEM((tokens, LANES), F32),
            pltpu.VMEM((RING, 16, LANES), F32),
            pltpu.VMEM((RING - 1, 3, tokens, LANES), F32),
            pltpu.VMEM((16, LANES), F32),
            pltpu.VMEM((RING * CORES, 16, LANES), F32),
            pltpu.VMEM((RING, 8, LANES), F32),
            pltpu.VMEM((RING, 8, LANES), F32),
            pltpu.VMEM((RING, 8, LANES), F32),
            pltpu.VMEM((RING, 8, LANES), F32),
            pltpu.VMEM((RING, tokens, half_cols), F32),
            pltpu.VMEM((tokens, half_cols), BF16),
            pltpu.VMEM((2, tokens, half_cols), BF16),
            pltpu.VMEM((2, tokens // 2, half_cols), BF16),
            pltpu.VMEM((2, tokens, half_cols), BF16),
            pltpu.VMEM((3, z_rows, vocab), F32),
            pltpu.VMEM((pieces, z_rows, LANES), BF16),
            pltpu.VMEM((2, pieces, z_rows, LANES), BF16),
            pltpu.VMEM((2, pieces, z_rows // 2, LANES), BF16),
            pltpu.VMEM((2, pieces, z_rows, LANES), BF16),
            pltpu.VMEM((tokens, half_cols), F32),
            pltpu.VMEM((z_rows, vocab), F32),
            pltpu.SemaphoreType.DMA((2 + width // 1024,)),
            pltpu.SemaphoreType.DMA((1,)),
            pltpu.SemaphoreType.DMA((Sems.sends,)),
            pltpu.SemaphoreType.DMA((Sems.total(),)),
        ],
        compiler_params=pltpu.CompilerParams(
            collective_id=0, has_side_effects=True, vmem_limit_bytes=66_000_000
        ),
        name="policy_step",
    )(
        hidden,
        head_weight,
        token_ids.reshape(rows, LANES),
        old_logprob.reshape(rows, LANES),
        rewards,
        lengths,
        group_ids,
        loss_scale.reshape(1),
    )
    return (loss.reshape(()), grad_hidden, grad_weight)


def solution(mesh):
    return jax.shard_map(
        shards,
        mesh=mesh,
        in_specs=(
            P("dp", None),
            P(None, "tensor"),
            P("dp"),
            P("dp"),
            P("dp"),
            P("dp"),
            P("dp"),
            P(),
        ),
        out_specs=(P(), P("dp", "tensor"), P("dp", "tensor")),
        check_vma=False,
    )
```
